32 devices in a mesh: seq: 16 (over z, y, core), mp: 2 (over x).
Axes of the slice: x: 2, y: 2, z: 4, core: 2. Of those that a mesh axis runs over, the one named last changes fastest.
Arguments:
- query: bfloat16 [4096, 3072], P('seq', 'mp'), may hold values from -4.5 to 4.5
- key: bfloat16 [4096, 3072], P('seq', 'mp'), may hold values from -4.5 to 4.5
- value: bfloat16 [4096, 3072], P('seq', 'mp'), may hold values from -6 to 6
- clip_lengths: int32 [4, 4], replicated, may hold values from 0 to 1024, as said below
Outputs:
- attended: bfloat16 [4096, 3072], P(('seq', 'mp'))
The draws below stay inside these ranges and needn't reach their ends.
Inputs may be any that keep to these rules, and one draw needn't show every extreme that they name: `clip_lengths`: each row sums to 1024; a clip slot may be empty; in some bucket one clip fills all 1024 tokens.
All inputs are finite; a program needn't handle non-finite values.
Results may differ from the reference program's by a relative error of at most 0.01.
Values may be sent and summed in bfloat16 or wider, within the bound.
A program may use at most 64 MiB of HBM per device.

```python
import jax
import jax.numpy as jnp
from jax import lax

HD = 128
PER = 4
D = 3072
MOST = 1024
BUCKETS = 4
TOKENS = 4096


def draw_query(key, part):
    base = jax.random.normal(jax.random.fold_in(key, 1), (TOKENS, D), jnp.float32)
    return jnp.clip(base, -4.5, 4.5).astype(jnp.bfloat16)


def draw_key(key, part):
    base = jax.random.normal(jax.random.fold_in(key, 2), (TOKENS, D), jnp.float32)
    return jnp.clip(base, -4.5, 4.5).astype(jnp.bfloat16)


def draw_clip_lengths(key, part):
    cuts = jax.random.randint(jax.random.fold_in(key, 21), (BUCKETS, PER - 1), 0, MOST + 1).astype(jnp.int32)
    cuts = jnp.sort(cuts, axis=1)
    zeros = jnp.zeros((BUCKETS, 1), jnp.int32)
    filled = jnp.full((BUCKETS, 1), MOST, jnp.int32)
    lengths = jnp.diff(jnp.concatenate([zeros, cuts, filled], axis=1), axis=1)
    chosen = jax.random.randint(jax.random.fold_in(key, 22), (), 0, BUCKETS).astype(jnp.int32)
    single = jnp.concatenate([filled, jnp.zeros((BUCKETS, PER - 1), jnp.int32)], axis=1)
    rows = jnp.arange(BUCKETS, dtype=jnp.int32)[:, None] == chosen
    return jnp.where(rows, single, lengths).astype(jnp.int32)


def level_of(stream_key, shape, shards, smallest, largest):
    def one(dim, parts):
        draws = jax.random.uniform(jax.random.fold_in(jax.random.fold_in(stream_key, 6), dim), (parts,), jnp.float32, smallest / len(shards), largest / len(shards))
        return jnp.repeat(jnp.exp(draws), shape[dim] // parts).reshape((-1,) + (1,) * (len(shape) - dim - 1))

    loudness = one(*shards[0])
    for cut in shards[1:]:
        loudness = loudness * one(*cut)
    return loudness


def noise(rng, extent, spread, limit, split=(), kind=jnp.bfloat16):
    drawn = jax.random.normal(rng, extent, jnp.float32) * spread
    if len(split) > 0:
        drawn = level_of(rng, extent, split, -0.22, 0.18) * drawn
    return jnp.clip(drawn, min=-limit, max=limit).astype(kind)


def setup_inputs(seed: int = 0) -> dict:
    key_list = jax.random.split(jax.random.key(seed), 5)
    return {
        "query": draw_query(jax.random.fold_in(key_list[4], 71), 0),
        "key": draw_key(jax.random.fold_in(key_list[4], 71), 0),
        "value": noise(key_list[2], (TOKENS, D), 1.0, 6.0, ((0, 16), (1, 2))),
        "clip_lengths": draw_clip_lengths(jax.random.fold_in(key_list[4], 71), 0),
    }


NEG = -1.0e30


def clip_of(places, ends):
    bucket = (places // MOST).astype(jnp.int32)
    offset = (places - bucket * MOST).astype(jnp.int32)
    hits = jnp.sum((offset[:, None, None] >= ends[None, :, :]).astype(jnp.int32), axis=2).astype(jnp.int32)
    pick = bucket[:, None] == jnp.arange(BUCKETS, dtype=jnp.int32)[None, :]
    inner = jnp.sum(jnp.where(pick, hits, 0), axis=1).astype(jnp.int32)
    return (bucket * PER + inner).astype(jnp.int32)


def reference(query, key, value, clip_lengths):
    heads = D // HD
    scale = 1.0 / (HD ** 0.5)
    ends = jnp.cumsum(clip_lengths, axis=1).astype(jnp.int32)
    clip_ids = clip_of(jnp.arange(TOKENS, dtype=jnp.int32), ends)
    block = min(512, MOST)
    outputs = []
    for bucket in range(BUCKETS):
        low = bucket * MOST
        k_part = key[low:low + MOST].reshape(MOST, heads, HD).astype(jnp.float32)
        v_part = value[low:low + MOST].reshape(MOST, heads, HD).astype(jnp.float32)
        k_ids = clip_ids[low:low + MOST]
        q_all = query[low:low + MOST].reshape(MOST // block, block, heads, HD)
        q_idx = k_ids.reshape(MOST // block, block)

        def one_block(items):
            q_part, q_ids = items
            score = jnp.einsum("qhd,khd->hqk", q_part.astype(jnp.float32), k_part,
                               precision=lax.Precision.HIGHEST) * scale
            keep = (q_ids[:, None] == k_ids[None, :])[None]
            score = jnp.where(keep, score, NEG)
            top = jnp.max(score, axis=-1, keepdims=True)
            weight = jnp.where(keep, jnp.exp(score - top), 0.0)
            total = jnp.sum(weight, axis=-1)
            weight_low = lax.optimization_barrier(weight.astype(jnp.bfloat16)).astype(jnp.float32)
            summed = jnp.einsum("hqk,khd->qhd", weight_low, v_part, precision=lax.Precision.HIGHEST)
            result = summed / jnp.transpose(total)[:, :, None]
            return result.reshape(block, D).astype(jnp.bfloat16)

        pieces = lax.map(one_block, (q_all, q_idx))
        outputs.append(pieces.reshape(MOST, D))
    return jnp.concatenate(outputs, axis=0)
```

```python
import functools

import jax
import jax.numpy as jnp
from jax import lax
from jax.experimental import pallas as pl
from jax.experimental.pallas import tpu as pltpu
from jax.sharding import PartitionSpec as P

HD = 128
NEG = -1e30
LOG2E = 1.4426950408889634
MESH = pl.DeviceIdType.MESH


def kernel(
    group, pair, mp, heads,
    lengths, query, key, value, out,
    q_buf, k_buf, v_buf, o_buf,
    q_in, k_in, v_in, o_in, q_out, k_out, v_out, o_out,
):
    rows = query.shape[0]
    part = rows // mp
    per_core = heads // pair
    others = group // pair
    slots = lengths.shape[1]
    seq_index = lax.axis_index("seq")
    mp_index = lax.axis_index("mp")
    bucket = seq_index // group
    place = lax.rem(seq_index, group)
    core = lax.rem(place, pair)
    chip = place // pair

    def peer(chip_step, core_step):
        there_chip = lax.rem(chip + chip_step, others)
        there_core = lax.rem(core + core_step, pair)
        return there_chip, there_core, bucket * group + there_chip * pair + there_core

    def columns(owner, head):
        return pl.ds(pl.multiple_of((owner * per_core + head) * HD, HD), HD)

    def slot(index):
        return pl.ds(pl.multiple_of(index * rows, rows), rows)

    def local_copies(head):
        mine = columns(core, head)
        return (
            pltpu.make_async_copy(query.at[:, mine], q_buf.at[head, slot(core), :], q_in.at[head, core]),
            pltpu.make_async_copy(key.at[:, mine], k_buf.at[head, slot(place), :], k_in.at[head, place]),
            pltpu.make_async_copy(value.at[:, mine], v_buf.at[head, slot(place), :], v_in.at[head, place]),
        )

    def sends(head, chip_step, core_step):
        there_chip, there_core, there_seq = peer(chip_step, core_step)
        theirs = columns(there_core, head)
        target = {"seq": there_seq, "mp": mp_index}
        index = chip_step * pair + core_step
        copies = [
            pltpu.make_async_remote_copy(
                src_ref=source.at[:, theirs], dst_ref=buf.at[head, slot(place), :],
                send_sem=left.at[head, index], recv_sem=landed.at[head, place],
                device_id=target, device_id_type=MESH,
            )
            for source, buf, left, landed in (
                (key, k_buf, k_out, k_in), (value, v_buf, v_out, v_in),
            )
        ]
        if chip_step == 0:
            copies.insert(0, pltpu.make_async_remote_copy(
                src_ref=query.at[:, theirs], dst_ref=q_buf.at[head, slot(core), :],
                send_sem=q_out.at[head, index], recv_sem=q_in.at[head, core],
                device_id=target, device_id_type=MESH,
            ))
        return copies

    def results(head, core_step, mp_step):
        there_core = lax.rem(core + core_step, pair)
        there_mp = lax.rem(mp_index + mp_step, mp)
        source = o_buf.at[head, pl.ds(pl.multiple_of(there_core * rows + there_mp * part, part), part), :]
        place_out = out.at[:, pl.ds(pl.multiple_of((mp_index * heads + core * per_core + head) * HD, HD), HD)]
        index = core_step * mp + mp_step
        if index == 0:
            return pltpu.make_async_copy(source, place_out, o_in.at[head, 0])
        return pltpu.make_async_remote_copy(
            src_ref=source, dst_ref=place_out,
            send_sem=o_out.at[head, index], recv_sem=o_in.at[head, index],
            device_id={"seq": bucket * group + chip * pair + there_core, "mp": there_mp},
            device_id_type=MESH,
        )

    far = [(a, b) for b in range(pair) for a in range(1, others)]
    near = [(0, b) for b in range(1, pair)]
    to_owner = [(b, m) for m in range(mp) for b in range(pair)]

    barrier = pltpu.get_barrier_semaphore()
    for chip_step, core_step in far + near:
        there_seq = peer(chip_step, core_step)[2]
        pl.semaphore_signal(barrier, inc=1, device_id={"seq": there_seq, "mp": mp_index}, device_id_type=MESH)
    for core_step, mp_step in to_owner:
        if mp_step > 0:
            pl.semaphore_signal(
                barrier, inc=1,
                device_id={"seq": peer(0, core_step)[2], "mp": lax.rem(mp_index + mp_step, mp)},
                device_id_type=MESH,
            )

    @pl.loop(0, per_core)
    def _(head):
        for copy in local_copies(head):
            copy.start()

    ends = []
    running = jnp.int32(0)
    for i in range(slots):
        running = running + lengths[bucket, i]
        ends.append(running)

    def ids(offset):
        found = jnp.zeros_like(offset)
        for end in ends:
            found = found + (offset >= end).astype(jnp.int32)
        return found

    k_ids = ids(lax.broadcasted_iota(jnp.int32, (1, group * rows), 1))

    pl.semaphore_wait(barrier, len(far) + len(near) + (mp - 1) * pair)

    @pl.loop(0, per_core)
    def _(head):
        together = [sends(head, *step) for step in far]
        for kind in range(2):
            for copies in together:
                copies[kind].start()
        for step in near:
            for copy in sends(head, *step):
                copy.start()

    def arrived(buf, sem, head, count):
        for i in range(count):
            ref = buf.at[head, pl.ds(i * rows, rows), :]
            pltpu.make_async_copy(ref, ref, sem.at[head, i]).wait()

    factor = LOG2E / HD**0.5

    @pl.loop(0, per_core)
    def _(head):
        arrived(q_buf, q_in, head, pair)
        arrived(k_buf, k_in, head, group)
        arrived(v_buf, v_in, head, group)
        keys = k_buf[head]
        values = v_buf[head]
        for b in range(pair):
            q_rows = q_buf[head, pl.ds(b * rows, rows), :]
            q_ids = ids(lax.broadcasted_iota(jnp.int32, (rows, 1), 0) + (chip * pair + b) * rows)
            score = lax.dot_general(
                q_rows, keys, (((1,), (1,)), ((), ())), preferred_element_type=jnp.float32
            )
            score = jnp.where(q_ids == k_ids, score, NEG)
            top = jnp.max(score, axis=1, keepdims=True)
            weight = jnp.exp2((score - top) * factor)
            total = jnp.sum(weight, axis=1, keepdims=True)
            summed = jnp.dot(weight.astype(jnp.bfloat16), values, preferred_element_type=jnp.float32)
            o_buf[head, pl.ds(b * rows, rows), :] = (summed / total).astype(jnp.bfloat16)
        for step in reversed(to_owner):
            results(head, *step).start()

    @pl.loop(0, per_core)
    def _(head):
        for step in far + near:
            for copy in sends(head, *step):
                copy.wait_send()
        for step in to_owner:
            if step == (0, 0):
                results(head, *step).wait()
            else:
                results(head, *step).wait_send()
                results(head, *step).wait_recv()


def shards(query, key, value, clip_lengths):
    rows, width = query.shape
    heads = width // HD
    group = lax.axis_size("seq") // clip_lengths.shape[0]
    mp = lax.axis_size("mp")
    pair = 2 if group % 2 == 0 and heads % 2 == 0 else 1
    per_core = heads // pair
    dma = pltpu.SemaphoreType.DMA
    whole = pl.BlockSpec(memory_space=pl.ANY)
    return pl.pallas_call(
        functools.partial(kernel, group, pair, mp, heads),
        out_shape=jax.ShapeDtypeStruct((rows // mp, width * mp), jnp.bfloat16),
        in_specs=[pl.BlockSpec(memory_space=pltpu.SMEM), whole, whole, whole],
        out_specs=pl.BlockSpec(memory_space=pltpu.VMEM),
        scratch_shapes=[
            pltpu.VMEM((per_core, pair * rows, HD), jnp.bfloat16),
            pltpu.VMEM((per_core, group * rows, HD), jnp.bfloat16),
            pltpu.VMEM((per_core, group * rows, HD), jnp.bfloat16),
            pltpu.VMEM((per_core, pair * rows, HD), jnp.bfloat16),
            dma((per_core, pair)), dma((per_core, group)), dma((per_core, group)), dma((per_core, pair * mp)),
            dma((per_core, pair)), dma((per_core, group)), dma((per_core, group)), dma((per_core, pair * mp)),
        ],
        compiler_params=pltpu.CompilerParams(collective_id=0, has_side_effects=True),
        name="packed_attention",
    )(clip_lengths, query, key, value)


def solution(mesh):
    in_specs = (P("seq", "mp"), P("seq", "mp"), P("seq", "mp"), P())
    out_specs = P(("seq", "mp"), None)
    return jax.shard_map(shards, mesh=mesh, in_specs=in_specs, out_specs=out_specs, check_vma=False)
```

```python
import functools

import jax
import jax.numpy as jnp
from jax import lax
from jax.experimental import pallas as pl
from jax.experimental.pallas import tpu as pltpu
from jax.sharding import PartitionSpec as P

HD = 128
NEG = -1e30
LOG2E = 1.4426950408889634
MESH = pl.DeviceIdType.MESH


def kernel(
    group, pair, mp, heads,
    lengths, query, key, value, out,
    q_buf, k_buf, v_buf, o_buf, k_first, v_first, p_buf, t_buf,
    q_in, k_in, v_in, o_in, q_out, k_out, v_out, o_out, first_in,
):
    rows = query.shape[0]
    part = rows // mp
    per_core = heads // pair
    others = group // pair
    slots = lengths.shape[1]
    seq_index = lax.axis_index("seq")
    mp_index = lax.axis_index("mp")
    bucket = seq_index // group
    place = lax.rem(seq_index, group)
    core = lax.rem(place, pair)
    chip = place // pair

    def seq_of(chip_step, there_core):
        return bucket * group + lax.rem(chip + chip_step, others) * pair + there_core

    def columns(owner, head):
        return pl.ds(pl.multiple_of((owner * per_core + head) * HD, HD), HD)

    def slot(index):
        return pl.ds(pl.multiple_of(index * rows, rows), rows)

    def local_copies(head):
        mine = columns(core, head)
        return (
            pltpu.make_async_copy(query.at[:, mine], q_buf.at[head, slot(core), :], q_in.at[head, core]),
            pltpu.make_async_copy(key.at[:, mine], k_buf.at[head, slot(place), :], k_in.at[head, place]),
            pltpu.make_async_copy(value.at[:, mine], v_buf.at[head, slot(place), :], v_in.at[head, place]),
        )

    def first_copies(there_core):
        theirs = columns(there_core, 0)
        return (
            pltpu.make_async_copy(key.at[:, theirs], k_first.at[there_core], first_in.at[0, there_core]),
            pltpu.make_async_copy(value.at[:, theirs], v_first.at[there_core], first_in.at[1, there_core]),
        )

    def send(head, chip_step, there_core, kind, staged=None):
        source, buf, left, landed = (
            (query, q_buf, q_out, q_in), (key, k_buf, k_out, k_in), (value, v_buf, v_out, v_in)
        )[kind]
        at = core if kind == 0 else place
        index = there_core if kind == 0 else chip_step * pair + there_core
        return pltpu.make_async_remote_copy(
            src_ref=source.at[:, columns(there_core, head)] if staged is None else staged.at[there_core],
            dst_ref=buf.at[head, slot(at), :],
            send_sem=left.at[head, index], recv_sem=landed.at[head, at],
            device_id={"seq": seq_of(chip_step, there_core), "mp": mp_index}, device_id_type=MESH,
        )

    def far_sends(head, staged=(None, None, None)):
        return [
            send(head, chip_step, there_core, kind, staged[kind])
            for kind in (1, 2) for there_core in range(pair) for chip_step in range(1, others)
        ]

    def near_sends(head):
        return [
            send(head, 0, lax.rem(core + step, pair), kind)
            for kind in range(3) for step in range(1, pair)
        ]

    def results(head, core_step, mp_step):
        there_core = lax.rem(core + core_step, pair)
        there_mp = lax.rem(mp_index + mp_step, mp)
        source = o_buf.at[head, pl.ds(pl.multiple_of(there_core * rows + there_mp * part, part), part), :]
        place_out = out.at[:, pl.ds(pl.multiple_of((mp_index * heads + core * per_core + head) * HD, HD), HD)]
        index = core_step * mp + mp_step
        if index == 0:
            return pltpu.make_async_copy(source, place_out, o_in.at[head, 0])
        return pltpu.make_async_remote_copy(
            src_ref=source, dst_ref=place_out,
            send_sem=o_out.at[head, index], recv_sem=o_in.at[head, index],
            device_id={"seq": seq_of(0, there_core), "mp": there_mp}, device_id_type=MESH,
        )

    for there_core in range(pair):
        for copy in first_copies(there_core):
            copy.start()

    barrier = pltpu.get_barrier_semaphore()
    greeted = [(seq_of(a, b), mp_index) for a in range(1, others) for b in range(pair)]
    greeted += [(seq_of(0, lax.rem(core + b, pair)), mp_index) for b in range(1, pair)]
    greeted += [(seq_of(0, b), lax.rem(mp_index + m, mp)) for b in range(pair) for m in range(1, mp)]
    for there_seq, there_mp in greeted:
        pl.semaphore_signal(
            barrier, inc=1, device_id={"seq": there_seq, "mp": there_mp}, device_id_type=MESH
        )

    @pl.loop(0, per_core)
    def _(head):
        for copy in local_copies(head):
            copy.start()

    ends = []
    running = jnp.int32(0)
    for i in range(slots):
        running = running + lengths[bucket, i]
        ends.append(running)

    def ids(offset):
        found = jnp.zeros_like(offset)
        for end in ends:
            found = found + (offset >= end).astype(jnp.int32)
        return found

    k_ids = ids(lax.broadcasted_iota(jnp.int32, (1, group * rows), 1))

    for there_core in range(pair):
        for copy in first_copies(there_core):
            copy.wait()
    pl.semaphore_wait(barrier, len(greeted))

    for copy in far_sends(0, (None, k_first, v_first)) + near_sends(0):
        copy.start()

    @pl.loop(1, per_core)
    def _(head):
        for copy in far_sends(head) + near_sends(head):
            copy.start()

    def arrived(buf, sem, head, count):
        for i in range(count):
            ref = buf.at[head, pl.ds(i * rows, rows), :]
            pltpu.make_async_copy(ref, ref, sem.at[head, i]).wait()

    factor = LOG2E / HD**0.5

    def settle(head):
        for step in range(pair * mp):
            copy = results(head, step // mp, step % mp)
            if step == 0:
                copy.wait()
            else:
                copy.wait_send()
                copy.wait_recv()

    @pl.loop(0, per_core)
    def _(head):
        arrived(q_buf, q_in, head, pair)
        arrived(k_buf, k_in, head, group)
        keys = k_buf[head]
        for b in range(pair):
            block = pl.ds(b * rows, rows)
            q_ids = ids(lax.broadcasted_iota(jnp.int32, (rows, 1), 0) + (chip * pair + b) * rows)
            score = lax.dot_general(
                q_buf[head, block, :], keys, (((1,), (1,)), ((), ())), preferred_element_type=jnp.float32
            )
            score = jnp.where(q_ids == k_ids, score, NEG)
            top = jnp.max(score, axis=1, keepdims=True)
            weight = jnp.exp2((score - top) * factor)
            t_buf[block, :] = jnp.broadcast_to(jnp.sum(weight, axis=1, keepdims=True), (rows, HD))
            p_buf[block, :] = weight.astype(jnp.bfloat16)
        arrived(v_buf, v_in, head, group)
        for core_step in reversed(range(pair)):
            block = slot(lax.rem(core + core_step, pair))
            summed = jnp.dot(p_buf[block, :], v_buf[head], preferred_element_type=jnp.float32)
            o_buf[head, block, :] = (summed / t_buf[block, :]).astype(jnp.bfloat16)
            for mp_step in reversed(range(mp)):
                results(head, core_step, mp_step).start()
        for copy in far_sends(head) + near_sends(head):
            copy.wait_send()

        @pl.when(head > 0)
        def _():
            settle(head - 1)

    settle(per_core - 1)


def shards(query, key, value, clip_lengths):
    rows, width = query.shape
    heads = width // HD
    group = lax.axis_size("seq") // clip_lengths.shape[0]
    mp = lax.axis_size("mp")
    pair = 2 if group % 2 == 0 and heads % 2 == 0 else 1
    per_core = heads // pair
    dma = pltpu.SemaphoreType.DMA
    whole = pl.BlockSpec(memory_space=pl.ANY)
    return pl.pallas_call(
        functools.partial(kernel, group, pair, mp, heads),
        out_shape=pltpu.VMEM((rows // mp, width * mp), jnp.bfloat16),
        in_specs=[pl.BlockSpec(memory_space=pltpu.SMEM), whole, whole, whole],
        out_specs=pl.BlockSpec(memory_space=pltpu.VMEM),
        scratch_shapes=[
            pltpu.VMEM((per_core, pair * rows, HD), jnp.bfloat16),
            pltpu.VMEM((per_core, group * rows, HD), jnp.bfloat16),
            pltpu.VMEM((per_core, group * rows, HD), jnp.bfloat16),
            pltpu.VMEM((per_core, pair * rows, HD), jnp.bfloat16),
            pltpu.VMEM((pair, rows, HD), jnp.bfloat16),
            pltpu.VMEM((pair, rows, HD), jnp.bfloat16),
            pltpu.VMEM((pair * rows, group * rows), jnp.bfloat16),
            pltpu.VMEM((pair * rows, HD), jnp.float32),
            dma((per_core, pair)), dma((per_core, group)), dma((per_core, group)), dma((per_core, pair * mp)),
            dma((per_core, pair)), dma((per_core, group)), dma((per_core, group)), dma((per_core, pair * mp)),
            dma((2, pair)),
        ],
        compiler_params=pltpu.CompilerParams(collective_id=0, has_side_effects=True),
        name="packed_attention",
    )(clip_lengths, query, key, value)


def solution(mesh):
    in_specs = (P("seq", "mp"), P("seq", "mp"), P("seq", "mp"), P())
    out_specs = P(("seq", "mp"), None)
    return jax.shard_map(shards, mesh=mesh, in_specs=in_specs, out_specs=out_specs, check_vma=False)
```

```python
import functools

import jax
import jax.numpy as jnp
from jax import lax
from jax.experimental import pallas as pl
from jax.experimental.pallas import tpu as pltpu
from jax.sharding import PartitionSpec as P

HD = 128
NEG = -1e30
LOG2E = 1.4426950408889634
MESH = pl.DeviceIdType.MESH


def kernel(
    group, pair, mp, heads, extra,
    lengths, query, key, value, out,
    q_buf, k_buf, v_buf, o_buf, first, p_buf, t_buf,
    q_in, k_in, v_in, o_in, q_out, k_out, v_out, o_out, first_in, ready,
):
    rows = query.shape[0]
    part = rows // mp
    per_core = heads // pair
    others = group // pair
    held = per_core - extra
    slots = lengths.shape[1]
    seq_index = lax.axis_index("seq")
    mp_index = lax.axis_index("mp")
    bucket = seq_index // group
    place = lax.rem(seq_index, group)
    core = lax.rem(place, pair)
    chip = place // pair

    def chip_at(chip_step):
        return lax.rem(chip + chip_step, others)

    def seq_of(chip_step, there_core):
        return bucket * group + chip_at(chip_step) * pair + there_core

    def head_of(slot, there_chip):
        if extra and isinstance(slot, int) and slot == 0:
            return there_chip
        return slot + extra

    def columns(owner, head):
        return pl.ds(pl.multiple_of((owner * per_core + head) * HD, HD), HD)

    def block_at(index):
        return pl.ds(pl.multiple_of(index * rows, rows), rows)

    kinds = ((query, q_buf, q_out, q_in), (key, k_buf, k_out, k_in), (value, v_buf, v_out, v_in))

    def local_copies(slot):
        mine = columns(core, head_of(slot, chip))
        return [
            pltpu.make_async_copy(source.at[:, mine], buf.at[slot, block_at(place), :], landed.at[slot, place])
            for source, buf, left, landed in kinds
        ]

    def far_kinds(slot):
        whole = extra and isinstance(slot, int) and slot == 0
        return (0, 1, 2) if whole else (1, 2)

    far = [(chip_step, there_core) for there_core in range(pair) for chip_step in range(1, others)]

    def first_copies():
        return [
            pltpu.make_async_copy(
                kinds[kind][0].at[:, columns(there_core, head_of(0, chip_at(chip_step)))],
                first.at[kind, chip_step * pair + there_core],
                first_in.at[kind, chip_step * pair + there_core],
            )
            for kind in far_kinds(0) for chip_step, there_core in far
        ]

    def send(slot, chip_step, there_core, kind, staged=False):
        source, buf, left, landed = kinds[kind]
        index = chip_step * pair + there_core
        if staged:
            origin = first.at[kind, index]
        else:
            origin = source.at[:, columns(there_core, head_of(slot, chip_at(chip_step)))]
        return pltpu.make_async_remote_copy(
            src_ref=origin, dst_ref=buf.at[slot, block_at(place), :],
            send_sem=left.at[slot, index], recv_sem=landed.at[slot, place],
            device_id={"seq": seq_of(chip_step, there_core), "mp": mp_index}, device_id_type=MESH,
        )

    def far_sends(slot, staged=False):
        return [send(slot, a, b, kind, staged) for kind in far_kinds(slot) for a, b in far]

    def near_sends(slot):
        return [
            send(slot, 0, lax.rem(core + step, pair), kind)
            for kind in range(3) for step in range(1, pair)
        ]

    def result(turn, slot, chip_step, core_step, mp_step):
        there_core = lax.rem(core + core_step, pair)
        there_mp = lax.rem(mp_index + mp_step, mp)
        source = o_buf.at[turn, pl.ds(pl.multiple_of(there_core * rows + there_mp * part, part), part), :]
        column = (mp_index * heads + core * per_core + head_of(slot, chip)) * HD
        target = out.at[:, pl.ds(pl.multiple_of(column, HD), HD)]
        index = core_step * mp + mp_step
        if chip_step == 0 and index == 0:
            return pltpu.make_async_copy(source, target, o_in.at[turn, index])
        return pltpu.make_async_remote_copy(
            src_ref=source, dst_ref=target, send_sem=o_out.at[turn, index], recv_sem=o_in.at[turn, index],
            device_id={"seq": seq_of(chip_step, there_core), "mp": there_mp}, device_id_type=MESH,
        )

    for copy in first_copies():
        copy.start()

    barrier = pltpu.get_barrier_semaphore()
    beside = [(seq_of(0, b), lax.rem(mp_index + m, mp)) for b in range(pair) for m in range(1, mp)]
    greeted = [(seq_of(a, b), mp_index) for a, b in far]
    greeted += [(seq_of(0, lax.rem(core + b, pair)), mp_index) for b in range(1, pair)]
    greeted += beside
    for there_seq, there_mp in greeted:
        pl.semaphore_signal(
            barrier, inc=1, device_id={"seq": there_seq, "mp": there_mp}, device_id_type=MESH
        )

    for copy in local_copies(0):
        copy.start()

    @pl.loop(1, held)
    def _(slot):
        for copy in local_copies(slot):
            copy.start()

    ends = []
    running = jnp.int32(0)
    for i in range(slots):
        running = running + lengths[bucket, i]
        ends.append(running)

    def ids(offset):
        found = jnp.zeros_like(offset)
        for end in ends:
            found = found + (offset >= end).astype(jnp.int32)
        return found

    k_ids = ids(lax.broadcasted_iota(jnp.int32, (1, group * rows), 1))

    for copy in first_copies():
        copy.wait()
    pl.semaphore_wait(barrier, len(greeted))

    for copy in far_sends(0, True) + near_sends(0):
        copy.start()

    @pl.loop(1, held)
    def _(slot):
        for copy in far_sends(slot) + near_sends(slot):
            copy.start()

    if extra:
        for there_seq, there_mp in beside:
            pl.semaphore_signal(
                ready, inc=1, device_id={"seq": there_seq, "mp": there_mp}, device_id_type=MESH
            )

    def arrived(kind, slot, base, count):
        buf, landed = kinds[kind][1], kinds[kind][3]
        for i in range(count):
            ref = buf.at[slot, block_at(base + i), :]
            pltpu.make_async_copy(ref, ref, landed.at[slot, base + i]).wait()

    factor = LOG2E / HD**0.5

    def weigh(slot, chip_step):
        keys = k_buf[slot]
        for b in range(pair):
            block = pl.ds(b * rows, rows)
            from_row = (chip_at(chip_step) * pair + b) * rows
            q_ids = ids(lax.broadcasted_iota(jnp.int32, (rows, 1), 0) + from_row)
            score = lax.dot_general(
                q_buf[slot, pl.ds(pl.multiple_of(from_row, rows), rows), :], keys,
                (((1,), (1,)), ((), ())), preferred_element_type=jnp.float32,
            )
            score = jnp.where(q_ids == k_ids, score, NEG)
            top = jnp.max(score, axis=1, keepdims=True)
            weight = jnp.exp2((score - top) * factor)
            t_buf[block, :] = jnp.broadcast_to(jnp.sum(weight, axis=1, keepdims=True), (rows, HD))
            p_buf[block, :] = weight.astype(jnp.bfloat16)

    def attend(turn, slot, chip_step):
        for core_step in reversed(range(pair)):
            block = block_at(lax.rem(core + core_step, pair))
            summed = jnp.dot(p_buf[block, :], v_buf[slot], preferred_element_type=jnp.float32)
            o_buf[turn, block, :] = (summed / t_buf[block, :]).astype(jnp.bfloat16)
            if chip_step == 0:
                for mp_step in reversed(range(mp)):
                    result(turn, slot, 0, core_step, mp_step).start()

    def far_results(mp_steps):
        return [
            result(a - 1, 0, a, core_step, mp_step)
            for mp_step in mp_steps for core_step in range(pair) for a in range(1, extra + 1)
        ]

    def settle(turn, slot, chip_step=0):
        for core_step in range(pair):
            for mp_step in range(mp):
                copy = result(turn, slot, chip_step, core_step, mp_step)
                if chip_step == 0 and core_step == 0 and mp_step == 0:
                    copy.wait()
                else:
                    copy.wait_send()
                    copy.wait_recv()

    begin = 0
    if extra:
        begin = 1
        arrived(0, 0, 0, group)
        arrived(1, 0, 0, group)
        for step in range(1, extra + 1):
            weigh(0, step)
            if step == 1:
                arrived(2, 0, 0, group)
            attend(step - 1, 0, step)
        weigh(0, 0)
        attend(extra, 0, 0)
        for copy in far_sends(0, True) + near_sends(0):
            copy.wait_send()

    @pl.loop(begin, held)
    def _(slot):
        arrived(0, slot, chip * pair, pair)
        arrived(1, slot, 0, group)
        if extra:
            @pl.when(slot == held - 1)
            def _():
                pl.semaphore_wait(ready, len(beside))
                for copy in far_results(list(range(1, mp)) + [0]):
                    copy.start()
        weigh(slot, 0)
        arrived(2, slot, 0, group)
        attend(slot + extra, slot, 0)
        for copy in far_sends(slot) + near_sends(slot):
            copy.wait_send()

        @pl.when(slot > begin)
        def _():
            settle(slot + extra - 1, slot - 1)

    if extra:
        settle(extra, 0)
    settle(held - 1 + extra, held - 1)
    for step in range(1, extra + 1):
        settle(step - 1, 0, step)


def shards(query, key, value, clip_lengths):
    rows, width = query.shape
    heads = width // HD
    group = lax.axis_size("seq") // clip_lengths.shape[0]
    mp = lax.axis_size("mp")
    pair = 2 if group % 2 == 0 and heads % 2 == 0 else 1
    per_core = heads // pair
    others = group // pair
    extra = others - 1 if per_core > others else 0
    held = per_core - extra
    dma = pltpu.SemaphoreType.DMA
    whole = pl.BlockSpec(memory_space=pl.ANY)
    return pl.pallas_call(
        functools.partial(kernel, group, pair, mp, heads, extra),
        out_shape=pltpu.VMEM((rows // mp, width * mp), jnp.bfloat16),
        in_specs=[pl.BlockSpec(memory_space=pltpu.SMEM), whole, whole, whole],
        out_specs=pl.BlockSpec(memory_space=pltpu.VMEM),
        scratch_shapes=[
            pltpu.VMEM((held, group * rows, HD), jnp.bfloat16),
            pltpu.VMEM((held, group * rows, HD), jnp.bfloat16),
            pltpu.VMEM((held, group * rows, HD), jnp.bfloat16),
            pltpu.VMEM((per_core, pair * rows, HD), jnp.bfloat16),
            pltpu.VMEM((3, group, rows, HD), jnp.bfloat16),
            pltpu.VMEM((pair * rows, group * rows), jnp.bfloat16),
            pltpu.VMEM((pair * rows, HD), jnp.float32),
            dma((held, group)), dma((held, group)), dma((held, group)), dma((per_core, pair * mp)),
            dma((held, group)), dma((held, group)), dma((held, group)), dma((per_core, pair * mp)),
            dma((3, group)), pltpu.SemaphoreType.REGULAR,
        ],
        compiler_params=pltpu.CompilerParams(collective_id=0, has_side_effects=True),
        name="packed_attention",
    )(clip_lengths, query, key, value)


def solution(mesh):
    in_specs = (P("seq", "mp"), P("seq", "mp"), P("seq", "mp"), P())
    out_specs = P(("seq", "mp"), None)
    return jax.shard_map(shards, mesh=mesh, in_specs=in_specs, out_specs=out_specs, check_vma=False)
```

```python
import functools

import jax
import jax.numpy as jnp
from jax import lax
from jax.experimental import pallas as pl
from jax.experimental.pallas import tpu as pltpu
from jax.sharding import PartitionSpec as P

HD = 128
NEG = -1e30
LOG2E = 1.4426950408889634
MESH = pl.DeviceIdType.MESH


def kernel(
    group, pair, mp, heads, lead,
    lengths, query, key, value, out,
    q_buf, k_buf, v_buf, o_buf, first, p_buf, t_buf,
    q_in, k_in, v_in, o_in, q_out, k_out, v_out, o_out, first_in, ready,
):
    rows = query.shape[0]
    part = rows // mp
    per_core = heads // pair
    others = group // pair
    extra = lead * (others - 1)
    held = per_core - extra
    slots = lengths.shape[1]
    seq_index = lax.axis_index("seq")
    mp_index = lax.axis_index("mp")
    bucket = seq_index // group
    place = lax.rem(seq_index, group)
    core = lax.rem(place, pair)
    chip = place // pair

    def chip_at(chip_step):
        return lax.rem(chip + chip_step, others)

    def seq_of(chip_step, there_core):
        return bucket * group + chip_at(chip_step) * pair + there_core

    def head_of(slot, there_chip):
        if isinstance(slot, int) and slot < lead:
            return slot * others + there_chip
        return slot + extra

    def columns(owner, head):
        return pl.ds(pl.multiple_of((owner * per_core + head) * HD, HD), HD)

    def block_at(index):
        return pl.ds(pl.multiple_of(index * rows, rows), rows)

    kinds = ((query, q_buf, q_out, q_in), (key, k_buf, k_out, k_in), (value, v_buf, v_out, v_in))

    def local_copies(slot):
        mine = columns(core, head_of(slot, chip))
        return [
            pltpu.make_async_copy(source.at[:, mine], buf.at[slot, block_at(place), :], landed.at[slot, place])
            for source, buf, left, landed in kinds
        ]

    def far_kinds(slot):
        whole = isinstance(slot, int) and slot < lead
        return (0, 1, 2) if whole else (1, 2)

    far = [(chip_step, there_core) for there_core in range(pair) for chip_step in range(1, others)]

    def first_copies():
        return [
            pltpu.make_async_copy(
                kinds[kind][0].at[:, columns(there_core, head_of(0, chip_at(chip_step)))],
                first.at[kind, chip_step * pair + there_core],
                first_in.at[kind, chip_step * pair + there_core],
            )
            for kind in far_kinds(0) for chip_step, there_core in far
        ]

    def send(slot, chip_step, there_core, kind, staged=False):
        source, buf, left, landed = kinds[kind]
        index = chip_step * pair + there_core
        if staged:
            origin = first.at[kind, index]
        else:
            origin = source.at[:, columns(there_core, head_of(slot, chip_at(chip_step)))]
        return pltpu.make_async_remote_copy(
            src_ref=origin, dst_ref=buf.at[slot, block_at(place), :],
            send_sem=left.at[slot, index], recv_sem=landed.at[slot, place],
            device_id={"seq": seq_of(chip_step, there_core), "mp": mp_index}, device_id_type=MESH,
        )

    def far_sends(slot, staged=False):
        return [send(slot, a, b, kind, staged) for kind in far_kinds(slot) for a, b in far]

    def near_sends(slot):
        return [
            send(slot, 0, lax.rem(core + step, pair), kind)
            for kind in range(3) for step in range(1, pair)
        ]

    def result(turn, slot, chip_step, core_step, mp_step):
        there_core = lax.rem(core + core_step, pair)
        there_mp = lax.rem(mp_index + mp_step, mp)
        source = o_buf.at[turn, pl.ds(pl.multiple_of(there_core * rows + there_mp * part, part), part), :]
        column = (mp_index * heads + core * per_core + head_of(slot, chip)) * HD
        target = out.at[:, pl.ds(pl.multiple_of(column, HD), HD)]
        index = core_step * mp + mp_step
        if chip_step == 0 and index == 0:
            return pltpu.make_async_copy(source, target, o_in.at[turn, index])
        return pltpu.make_async_remote_copy(
            src_ref=source, dst_ref=target, send_sem=o_out.at[turn, index], recv_sem=o_in.at[turn, index],
            device_id={"seq": seq_of(chip_step, there_core), "mp": there_mp}, device_id_type=MESH,
        )

    for copy in first_copies():
        copy.start()

    barrier = pltpu.get_barrier_semaphore()
    beside = [(seq_of(0, b), lax.rem(mp_index + m, mp)) for b in range(pair) for m in range(1, mp)]
    greeted = [(seq_of(a, b), mp_index) for a, b in far]
    greeted += [(seq_of(0, lax.rem(core + b, pair)), mp_index) for b in range(1, pair)]
    greeted += beside
    for there_seq, there_mp in greeted:
        pl.semaphore_signal(
            barrier, inc=1, device_id={"seq": there_seq, "mp": there_mp}, device_id_type=MESH
        )

    for slot in range(max(lead, 1)):
        for copy in local_copies(slot):
            copy.start()

    @pl.loop(max(lead, 1), held)
    def _(slot):
        for copy in local_copies(slot):
            copy.start()

    ends = []
    running = jnp.int32(0)
    for i in range(slots):
        running = running + lengths[bucket, i]
        ends.append(running)

    def ids(offset):
        found = jnp.zeros_like(offset)
        for end in ends:
            found = found + (offset >= end).astype(jnp.int32)
        return found

    k_ids = ids(lax.broadcasted_iota(jnp.int32, (1, group * rows), 1))

    for copy in first_copies():
        copy.wait()
    pl.semaphore_wait(barrier, len(greeted))

    for slot in range(max(lead, 1)):
        for copy in far_sends(slot, slot == 0) + near_sends(slot):
            copy.start()

    @pl.loop(max(lead, 1), held)
    def _(slot):
        for copy in far_sends(slot) + near_sends(slot):
            copy.start()

    if lead:
        for there_seq, there_mp in beside:
            pl.semaphore_signal(
                ready, inc=1, device_id={"seq": there_seq, "mp": there_mp}, device_id_type=MESH
            )

    def arrived(kind, slot, base, count):
        buf, landed = kinds[kind][1], kinds[kind][3]
        for i in range(count):
            ref = buf.at[slot, block_at(base + i), :]
            pltpu.make_async_copy(ref, ref, landed.at[slot, base + i]).wait()

    factor = LOG2E / HD**0.5

    def weigh(slot, chip_step):
        keys = k_buf[slot]
        for b in range(pair):
            block = pl.ds(b * rows, rows)
            from_row = (chip_at(chip_step) * pair + b) * rows
            q_ids = ids(lax.broadcasted_iota(jnp.int32, (rows, 1), 0) + from_row)
            score = lax.dot_general(
                q_buf[slot, pl.ds(pl.multiple_of(from_row, rows), rows), :], keys,
                (((1,), (1,)), ((), ())), preferred_element_type=jnp.float32,
            )
            score = jnp.where(q_ids == k_ids, score, NEG)
            top = jnp.max(score, axis=1, keepdims=True)
            weight = jnp.exp2((score - top) * factor)
            t_buf[block, :] = jnp.broadcast_to(jnp.sum(weight, axis=1, keepdims=True), (rows, HD))
            p_buf[block, :] = weight.astype(jnp.bfloat16)

    def attend(turn, slot, chip_step):
        for core_step in reversed(range(pair)):
            block = block_at(lax.rem(core + core_step, pair))
            summed = jnp.dot(p_buf[block, :], v_buf[slot], preferred_element_type=jnp.float32)
            o_buf[turn, block, :] = (summed / t_buf[block, :]).astype(jnp.bfloat16)
            if chip_step == 0:
                for mp_step in reversed(range(mp)):
                    result(turn, slot, 0, core_step, mp_step).start()

    def far_results(mp_steps):
        return [
            result(slot * (others - 1) + a - 1, slot, a, core_step, mp_step)
            for slot in range(lead) for mp_step in mp_steps
            for core_step in range(pair) for a in range(1, others)
        ]

    def settle(turn, slot, chip_step=0):
        for core_step in range(pair):
            for mp_step in range(mp):
                copy = result(turn, slot, chip_step, core_step, mp_step)
                if chip_step == 0 and core_step == 0 and mp_step == 0:
                    copy.wait()
                else:
                    copy.wait_send()
                    copy.wait_recv()

    for slot in range(lead):
        arrived(0, slot, 0, group)
        arrived(1, slot, 0, group)
        for step in range(1, others):
            weigh(slot, step)
            if step == 1:
                arrived(2, slot, 0, group)
            attend(slot * (others - 1) + step - 1, slot, step)
        weigh(slot, 0)
        attend(slot + extra, slot, 0)
        for copy in far_sends(slot, slot == 0) + near_sends(slot):
            copy.wait_send()
    if lead:
        pl.semaphore_wait(ready, len(beside))
        for copy in far_results(list(range(1, mp)) + [0]):
            copy.start()

    @pl.loop(lead, held)
    def _(slot):
        arrived(0, slot, chip * pair, pair)
        arrived(1, slot, 0, group)
        weigh(slot, 0)
        arrived(2, slot, 0, group)
        attend(slot + extra, slot, 0)
        for copy in far_sends(slot) + near_sends(slot):
            copy.wait_send()

        @pl.when(slot > lead)
        def _():
            settle(slot + extra - 1, slot - 1)

    for slot in range(lead):
        settle(slot + extra, slot)
    settle(held - 1 + extra, held - 1)
    for slot in range(lead):
        for step in range(1, others):
            settle(slot * (others - 1) + step - 1, slot, step)


def shards(query, key, value, clip_lengths):
    rows, width = query.shape
    heads = width // HD
    group = lax.axis_size("seq") // clip_lengths.shape[0]
    mp = lax.axis_size("mp")
    pair = 2 if group % 2 == 0 and heads % 2 == 0 else 1
    per_core = heads // pair
    others = group // pair
    lead = min(2, (per_core - 1) // others) if others > 1 else 0
    held = per_core - lead * (others - 1)
    dma = pltpu.SemaphoreType.DMA
    whole = pl.BlockSpec(memory_space=pl.ANY)
    return pl.pallas_call(
        functools.partial(kernel, group, pair, mp, heads, lead),
        out_shape=pltpu.VMEM((rows // mp, width * mp), jnp.bfloat16),
        in_specs=[pl.BlockSpec(memory_space=pltpu.SMEM), whole, whole, whole],
        out_specs=pl.BlockSpec(memory_space=pltpu.VMEM),
        scratch_shapes=[
            pltpu.VMEM((held, group * rows, HD), jnp.bfloat16),
            pltpu.VMEM((held, group * rows, HD), jnp.bfloat16),
            pltpu.VMEM((held, group * rows, HD), jnp.bfloat16),
            pltpu.VMEM((per_core, pair * rows, HD), jnp.bfloat16),
            pltpu.VMEM((3, group, rows, HD), jnp.bfloat16),
            pltpu.VMEM((pair * rows, group * rows), jnp.bfloat16),
            pltpu.VMEM((pair * rows, HD), jnp.float32),
            dma((held, group)), dma((held, group)), dma((held, group)), dma((per_core, pair * mp)),
            dma((held, group)), dma((held, group)), dma((held, group)), dma((per_core, pair * mp)),
            dma((3, group)), pltpu.SemaphoreType.REGULAR,
        ],
        compiler_params=pltpu.CompilerParams(collective_id=0, has_side_effects=True),
        name="packed_attention",
    )(clip_lengths, query, key, value)


def solution(mesh):
    in_specs = (P("seq", "mp"), P("seq", "mp"), P("seq", "mp"), P())
    out_specs = P(("seq", "mp"), None)
    return jax.shard_map(shards, mesh=mesh, in_specs=in_specs, out_specs=out_specs, check_vma=False)
```
